32 devices in a mesh: gx: 8 (over y, x, core), gy: 4 (over z).
Axes of the slice: x: 2, y: 2, z: 4, core: 2. Of those that a mesh axis runs over, the one named last changes fastest.
Arguments:
- probes: bfloat16 [256, 1024, 256], P('gx', 'gy'), may hold values from -6 to 6
- blk_rows: int32 [1024, 128], P(('gx', 'gy')), may hold values from 0 to 8191
- blk_sensor: int32 [1024], P(('gx', 'gy')), may hold values from 0 to 255, as said below
- blk_count: int32 [32], P(('gx', 'gy')), may hold values from 16 to 32, as said below
- coef: bfloat16 [1024, 128], P(('gx', 'gy')), may hold values from -5 to 5
- owner: int32 [256], replicated, may hold values from 0 to 31, as said below
- weights: float32 [256], replicated, may hold values from 0.1 to 1
Outputs:
- sensitivity: float32 [256], P(('gx', 'gy'))
- new_weights: float32 [256], replicated
- density: float32 [256, 1024], P('gx', 'gy')
The draws below stay inside these ranges and needn't reach their ends.
Inputs may be any that keep to these rules, and one draw needn't show every extreme that they name: `owner`: every device owns exactly 8 sensors. `blk_sensor`: among the live slots of one tile, at most 2 belong to sensors of one owner; in every draw some owner receives 2 live blocks from every tile. `blk_count`: some tile has all 32 slots live.
All inputs are finite; a program needn't handle non-finite values.
Results may differ from the reference program's by a relative error of at most 0.0008.
Values may be sent and summed in bfloat16 or wider, within the bound.
A program may use at most 128 MiB of HBM per device.

```python
import math
import jax
import jax.numpy as jnp
from jax import lax

P_SIZE = 256
FOOT = 128
TR = 32
TC = 256
SPD = 8
CAP = 2
SENSORS = 256
NBLK = 32
GR = 256
GC = 1024
N_GX = 8
N_GY = 4
DEVICES = 32


def layout(key):
    perm = jax.random.permutation(jax.random.fold_in(key, 11), SENSORS).astype(jnp.int32)
    owners = perm // SPD
    inverse = jnp.argsort(perm, stable=True).astype(jnp.int32)
    hot = jax.random.permutation(jax.random.fold_in(key, 12), DEVICES)[:2].astype(jnp.int32)
    entries = jnp.arange(DEVICES * CAP, dtype=jnp.int32)
    is_hot = jnp.any((entries // CAP)[:, None] == hot[None, :], axis=1).astype(jnp.int32)
    score = jax.random.randint(jax.random.fold_in(key, 13), (DEVICES, DEVICES * CAP), 0, 2 ** 20, dtype=jnp.int32)
    score = (score + is_hot[None, :] * 2 ** 21) * (DEVICES * CAP) + entries[None, :]
    chosen = lax.top_k(score, NBLK)[1].astype(jnp.int32)
    dest = chosen // CAP
    within = jax.random.randint(jax.random.fold_in(key, 14), (DEVICES, NBLK), 0, SPD, dtype=jnp.int32)
    sensor = inverse[dest * SPD + within]
    count = jax.random.randint(jax.random.fold_in(key, 15), (DEVICES,), NBLK // 2, NBLK + 1, dtype=jnp.int32)
    full_tile = jax.random.randint(jax.random.fold_in(key, 16), (), 0, DEVICES, dtype=jnp.int32)
    count = jnp.where(jnp.arange(DEVICES, dtype=jnp.int32) == full_tile, NBLK, count)
    return (owners, sensor.reshape(-1), count)


def draw_owner(key, part):
    return layout(key)[0]


def draw_blk_sensor(key, part):
    return layout(key)[1]


def draw_blk_count(key, part):
    return layout(key)[2]


def touch_ends(values, own_key, least, top_value):
    longest = values.shape.index(max(values.shape))
    spots = []
    for shift in (0, 1):
        where = [jax.random.randint(jax.random.fold_in(own_key, axis), (), 0, length) for axis, length in enumerate(values.shape)]
        where[longest] = (where[longest] + shift) % values.shape[longest]
        spots.append(tuple(where))
    return values.at[spots[0]].set(least).at[spots[1]].set(top_value)


def block_levels(key, dims, shards, smallest, high):
    loudness = 1.0
    for position, blocks in shards:
        steps = jax.random.uniform(jax.random.fold_in(jax.random.fold_in(key, 6), position), (blocks,), jnp.float32, smallest / len(shards), high / len(shards))
        loudness = loudness * jnp.repeat(jnp.exp(steps), dims[position] // blocks).reshape((-1,) + (1,) * (len(dims) - 1 - position))
    return loudness


def normal_values(key, extent, deviation, limit, cuts=(), kind=jnp.bfloat16):
    values = deviation * jax.random.normal(key, extent, jnp.float32)
    if cuts:
        values = values * block_levels(key, extent, cuts, -0.22, 0.18)
    return jnp.clip(values, -limit, limit).astype(kind)


def setup_inputs(seed: int = 0) -> dict:
    keys = jax.random.split(jax.random.key(seed), 8)
    return {
        "probes": normal_values(keys[0], (GR, GC, P_SIZE), 1.0, 6.0, ((0, 8), (1, 4))),
        "blk_rows": touch_ends(jax.random.randint(keys[1], (DEVICES * NBLK, FOOT), 0, TR * TC), jax.random.fold_in(keys[1], 1), 0, (TR * TC) - 1).astype(jnp.int32),
        "blk_sensor": draw_blk_sensor(jax.random.fold_in(keys[7], 71), 0),
        "blk_count": draw_blk_count(jax.random.fold_in(keys[7], 71), 0),
        "coef": normal_values(keys[4], (DEVICES * NBLK, FOOT), 1.0, 5.0, ((0, 32),)),
        "owner": draw_owner(jax.random.fold_in(keys[7], 71), 0),
        "weights": jnp.clip(jnp.exp(jax.random.uniform(keys[6], (SENSORS,), jnp.float32, math.log(0.1), math.log(1.0))), 0.1, 1.0),
    }


def reference(probes, blk_rows, blk_sensor, blk_count, coef, owner, weights):
    tiles = probes.reshape(N_GX, TR, N_GY, TC, P_SIZE).transpose(0, 2, 1, 3, 4).reshape(N_GX * N_GY, TR * TC, P_SIZE)
    rows = blk_rows.reshape(DEVICES, NBLK, FOOT)
    sensors = blk_sensor.reshape(DEVICES, NBLK)
    coefs = coef.reshape(DEVICES, NBLK, FOOT)
    live = (jnp.arange(NBLK, dtype=jnp.int32)[None, :] < blk_count[:, None]).astype(jnp.float32)

    def accumulate(obs, inputs):
        tile, row_ids, sens, weight, alive = inputs
        picked = tile[row_ids.reshape(-1)].reshape(NBLK, FOOT, P_SIZE).astype(jnp.float32)
        contrib = weight.astype(jnp.float32)[:, :, None] * picked * alive[:, None, None]
        return (obs.at[sens].add(contrib), None)
    obs = lax.scan(accumulate, jnp.zeros((SENSORS, FOOT, P_SIZE), jnp.float32), (tiles, rows, sensors, coefs, live))[0]
    sens_h = lax.optimization_barrier(jnp.sum(obs * obs, axis=(1, 2))) / (FOOT * P_SIZE)
    order = jnp.argsort(owner * SENSORS + jnp.arange(SENSORS, dtype=jnp.int32))
    sensitivity = sens_h[order]
    gain = weights * jnp.sqrt(1.0 + sens_h)
    new_weights = SENSORS * gain / jnp.sum(gain)
    values = live[:, :, None] * new_weights[sensors][:, :, None] * jnp.square(coefs.astype(jnp.float32))
    tile_ids = jnp.broadcast_to(jnp.arange(DEVICES, dtype=jnp.int32)[:, None, None], rows.shape)
    dens = jnp.zeros((DEVICES, TR * TC), jnp.float32).at[tile_ids, rows].add(values)
    density = dens.reshape(N_GX, N_GY, TR, TC).transpose(0, 2, 1, 3).reshape(N_GX * TR, N_GY * TC)
    return (sensitivity, new_weights, density)
```

```python
import functools

import jax
import jax.numpy as jnp
from jax import lax
from jax.experimental import pallas as pl
from jax.experimental.pallas import tpu as pltpu
from jax.sharding import PartitionSpec as P

MESH = pl.DeviceIdType.MESH
F32 = jnp.float32
BF16 = jnp.bfloat16
NT = (((1,), (1,)), ((), ()))
LANES = 128
LAG = 3
AHEAD = 3


def step_kernel(
    n_gx, n_gy, scale, tail,
    rows_hbm, probes_hbm, count_ref, sensor_ref, rows_ref, coef_ref, owner_ref, weights_ref,
    owned_ref, new_ref, density_ref,
    rows_sm, probes_ref, tile_ref, stage_ref, coef32_ref, send_ref, recv_ref, ids_send, ids_recv,
    mixer_ref, y_ref, part_out, part_in, part_x, acc_ref, planes_ref, h_send, h_recv,
    rows_sem, load_sem, send_sem, recv_sem, ids_send_sem, ids_recv_sem, part_send_sem,
    part_sem, part_x_sem, h_send_sem, h_recv_sem,
):
    n = n_gx * n_gy
    gx = lax.axis_index("gx")
    gy = lax.axis_index("gy")
    flat = gx * n_gy + gy
    items, _, nblk, width = send_ref.shape[1:]
    tile_r, tile_c, probe_n = probes_ref.shape
    split = probe_n // width
    groups = items // split
    depth_k = n_gx * nblk
    n_sens = owner_ref.shape[1]
    foot = coef_ref.shape[1]
    wide = ids_send.shape[1]
    share = wide // nblk
    first_tail = items - tail

    parts = load_sem.shape[0]
    span = tile_r // parts

    def load(q):
        at = pl.ds(q * span, span)
        return pltpu.make_async_copy(probes_hbm.at[at], probes_ref.at[at], load_sem.at[q])

    for q in range(parts):
        load(q).start()
    rows_copy = pltpu.make_async_copy(rows_hbm, rows_sm, rows_sem)
    rows_copy.start()

    def across(j):
        return (lax.rem(gx + j, n_gx), gy)

    barrier = pltpu.get_barrier_semaphore()

    def greet(j, carry):
        pl.semaphore_signal(barrier, inc=1, device_id=across(j), device_id_type=MESH)
        return carry

    lax.fori_loop(1, n_gx, greet, 0)

    @pl.when(gy > 0)
    def _():
        pl.semaphore_signal(barrier, inc=1, device_id=(gx, gy - 1), device_id_type=MESH)

    @pl.when(gy < n_gy - 1)
    def _():
        pl.semaphore_signal(barrier, inc=1, device_id=(gx, gy + 1), device_id_type=MESH)

    coef32_ref[...] = coef_ref[...].astype(F32)
    slot = lax.broadcasted_iota(jnp.int32, (1, nblk), 1)
    ids_one = jnp.where(slot < count_ref[...], sensor_ref[...] + 1, 0).astype(F32)
    down = lax.broadcasted_iota(jnp.int32, (nblk, nblk), 0)
    ids_col = jnp.sum(
        jnp.where(down == lax.broadcasted_iota(jnp.int32, (nblk, nblk), 1), ids_one, 0.0),
        axis=1, keepdims=True,
    )
    offset = lax.rem(gx, share) * nblk
    ids_send[...] = jnp.sum(
        jnp.where(
            lax.broadcasted_iota(jnp.int32, (nblk, wide), 1)
            == lax.broadcasted_iota(jnp.int32, (nblk, wide), 0) + offset,
            ids_col, 0.0,
        ),
        axis=0, keepdims=True,
    )
    ids_recv[gx] = ids_send[...]

    for q in range(parts):
        load(q).wait()

        def widen(i, carry):
            at = pl.multiple_of(i * tile_c, tile_c)
            tile_ref[pl.ds(at, tile_c), :] = probes_ref[i].astype(F32)
            return carry

        lax.fori_loop(q * span, (q + 1) * span, widen, 0)
    rows_copy.wait()

    def block_copy(q, c, j):
        return pltpu.make_async_remote_copy(
            src_ref=send_ref.at[q, c, across(j)[0]], dst_ref=recv_ref.at[q, c, gx],
            send_sem=send_sem.at[q, c], recv_sem=recv_sem.at[q, c],
            device_id=across(j), device_id_type=MESH,
        )

    def ids_copy(j):
        return pltpu.make_async_remote_copy(
            src_ref=ids_send, dst_ref=ids_recv.at[gx],
            send_sem=ids_send_sem.at[j], recv_sem=ids_recv_sem.at[gx],
            device_id=across(j), device_id_type=MESH,
        )

    def part_copy(q, c, up):
        return pltpu.make_async_remote_copy(
            src_ref=part_out.at[q, c], dst_ref=part_in.at[q, c],
            send_sem=part_send_sem.at[q, c], recv_sem=part_sem.at[q, c],
            device_id=(gx, gy + up), device_id_type=MESH,
        )

    def part_x_copy(q, c, up):
        return pltpu.make_async_remote_copy(
            src_ref=part_out.at[q, c], dst_ref=part_x.at[q, c - first_tail],
            send_sem=part_send_sem.at[q, c], recv_sem=part_x_sem.at[q, c - first_tail],
            device_id=(gx, gy + up), device_id_type=MESH,
        )

    def h_peer(k):
        t = lax.rem(flat + k, n)
        return t, (t // n_gy, lax.rem(t, n_gy))

    def h_copy(k):
        return pltpu.make_async_remote_copy(
            src_ref=h_send, dst_ref=h_recv.at[flat],
            send_sem=h_send_sem.at[k], recv_sem=h_recv_sem.at[flat],
            device_id=h_peer(k)[1], device_id_type=MESH,
        )

    channel = lax.broadcasted_iota(jnp.int32, (nblk, foot), 1)
    batch = stage_ref.shape[0]

    def gather(g):
        for q in range(2):
            def some(b, carry):
                for e in range(batch):
                    d = b * batch + e
                    r = (g * 2 + q) * n_gx + d
                    for j in range(nblk):
                        stage_ref[e, pl.ds(j, 1), :] = tile_ref[pl.ds(rows_sm[j, r], 1), :]
                    column = jnp.sum(
                        jnp.where(channel == r, coef32_ref[...], 0.0), axis=1, keepdims=True
                    )
                    block = (stage_ref[e] * column).astype(BF16)
                    for p in range(split):
                        send_ref[q, g * split + p, d] = block[:, p * width : (p + 1) * width]
                return carry

            lax.fori_loop(0, n_gx // batch, some, 0)

    def launch(g):
        for p in range(split):
            for q in range(2):
                c = g * split + p
                recv_ref[q, c, gx] = send_ref[q, c, gx]
                for j in range(1, n_gx):
                    block_copy(q, c, j).start()

    gather(0)
    pl.semaphore_wait(
        barrier,
        n_gx - 1 + jnp.where(gy > 0, 1, 0) + jnp.where(gy < n_gy - 1, 1, 0),
    )
    for j in range(1, n_gx):
        ids_copy(j).start()
    launch(0)

    def gather_on(g, carry):
        gather(g)
        launch(g)
        return carry

    lax.fori_loop(1, AHEAD, gather_on, 0)

    for j in range(1, n_gx):
        t = across(j)[0]
        pltpu.make_async_copy(ids_send, ids_recv.at[t], ids_recv_sem.at[t]).wait()
    sensor_up = (lax.broadcasted_iota(jnp.int32, (n_sens, wide), 0) + 1).astype(F32)
    for piece in range(n_gx // share):
        row = ids_recv[piece * share]
        for extra in range(1, share):
            row = row + ids_recv[piece * share + extra]
        mixer_ref[:, piece * wide : (piece + 1) * wide] = jnp.where(
            row == sensor_up, 1.0, 0.0
        ).astype(BF16)
    acc_ref[...] = jnp.zeros_like(acc_ref)

    others = pl.ds(0, n_gx - 1)

    def process(q, c, f, crossing):
        pltpu.make_async_copy(
            send_ref.at[q, c, others], recv_ref.at[q, c, others], recv_sem.at[q, c]
        ).wait()
        y_ref[...] = jnp.dot(
            mixer_ref[...], recv_ref[q, c].reshape(depth_k, width), preferred_element_type=F32
        )
        below = (gy > 0) & (gy <= f)
        above = (gy < n_gy - 1) & (gy >= f)

        @pl.when(below if q == 0 else above)
        def _():
            pltpu.make_async_copy(part_out.at[q, c], part_in.at[q, c], part_sem.at[q, c]).wait()
            y_ref[...] += part_in[q, c].astype(F32)

        if crossing:
            @pl.when(above if q == 0 else below)
            def _():
                at = c - first_tail
                pltpu.make_async_copy(
                    part_out.at[q, c], part_x.at[q, at], part_x_sem.at[q, at]
                ).wait()
                y_ref[...] += part_x[q, at].astype(F32)

        @pl.when(gy == f)
        def _():
            total = acc_ref[...]
            for at in range(0, width, LANES):
                y = y_ref[:, at : at + LANES]
                total = total + y * y
            acc_ref[...] = total

        @pl.when(gy < f)
        def _():
            part_out[q, c] = y_ref[...].astype(BF16)
            (part_copy if q == 0 else part_x_copy)(q, c, 1).start()

        @pl.when(gy > f)
        def _():
            part_out[q, c] = y_ref[...].astype(BF16)
            (part_copy if q == 1 else part_x_copy)(q, c, -1).start()

    def ends(q, crossing):
        if crossing:
            return n_gy // 2 - q
        return n_gy - 1 if q == 0 else 0

    def depth_of(f):
        low = jnp.where(gy <= f, gy, 0)
        high = jnp.where(gy >= f, n_gy - 1 - gy, 0)
        return jnp.maximum(low, high)

    def plane(j):
        at = rows_ref[pl.ds(j, 1), :]
        c = coef32_ref[pl.ds(j, 1), :]
        square = c * c
        top = square.astype(BF16).astype(F32)
        high = at // tile_c
        low = at - high * tile_c
        here = high == lax.broadcasted_iota(jnp.int32, (tile_r, foot), 0)
        left = jnp.concatenate(
            [jnp.where(here, top, 0.0), jnp.where(here, square - top, 0.0)], axis=0
        ).astype(BF16)
        right = jnp.where(
            low == lax.broadcasted_iota(jnp.int32, (tile_c, foot), 0), 1.0, 0.0
        ).astype(BF16)
        both = lax.dot_general(left, right, NT, preferred_element_type=F32)
        planes_ref[j] = both[:tile_r] + both[tile_r:]

    steps = items + LAG * (n_gy - 1)
    per_step = -(-nblk // items)

    def step(s, carry):
        g = s // split + AHEAD

        @pl.when((lax.rem(s, split) == 0) & (g < groups))
        def _():
            gather(g)
            launch(g)

        for crossing in (True, False):
            for q in range(2):
                f = ends(q, crossing)
                if crossing:
                    lo, hi = first_tail, items
                else:
                    lo, hi = 0, first_tail
                if lo == hi:
                    continue
                c = s - LAG * depth_of(f)

                @pl.when((c >= lo) & (c < hi))
                def _():
                    process(q, c, f, crossing)

        for e in range(per_step):
            @pl.when(s * per_step + e < nblk)
            def _():
                plane(s * per_step + e)

        return carry

    lax.fori_loop(0, steps, step, 0)

    eye = lax.broadcasted_iota(jnp.int32, (LANES, LANES), 0) == lax.broadcasted_iota(
        jnp.int32, (LANES, LANES), 1
    )
    for b in range(n_sens // LANES):
        s = jnp.sum(acc_ref[b * LANES : (b + 1) * LANES, :], axis=1, keepdims=True)
        h_send[:, b * LANES : (b + 1) * LANES] = jnp.sum(
            jnp.where(eye, s, 0.0), axis=0, keepdims=True
        )
    h_recv[flat] = h_send[...]

    def h_launch(k, carry):
        h_copy(k).start()
        return carry

    lax.fori_loop(1, n, h_launch, 0)

    spd = n_sens // n
    mine = jnp.where(owner_ref[...] == flat, 1.0, 0.0)
    before = jnp.where(
        lax.broadcasted_iota(jnp.int32, (n_sens, n_sens), 0)
        < lax.broadcasted_iota(jnp.int32, (n_sens, n_sens), 1),
        1.0, 0.0,
    ).astype(BF16)
    rank = jnp.dot(
        jnp.broadcast_to(mine, (spd, n_sens)).astype(BF16), before, preferred_element_type=F32
    )
    place = lax.broadcasted_iota(jnp.int32, (spd, n_sens), 0).astype(F32)
    select = jnp.where(rank == place, 1.0, 0.0) * mine

    def drain(c, carry):
        for q in range(2):
            pltpu.make_async_copy(
                send_ref.at[q, c, others], recv_ref.at[q, c, others], send_sem.at[q, c]
            ).wait()
            f = jnp.where(c < first_tail, ends(q, False), ends(q, True))

            @pl.when(gy != f)
            def _():
                pltpu.make_async_copy(
                    part_out.at[q, c], part_in.at[q, c], part_send_sem.at[q, c]
                ).wait()
        return carry

    lax.fori_loop(0, items, drain, 0)
    for j in range(1, n_gx):
        ids_copy(j).wait_send()

    def h_wait(k, carry):
        t = h_peer(k)[0]
        pltpu.make_async_copy(h_send, h_recv.at[t], h_recv_sem.at[t]).wait()
        return carry

    lax.fori_loop(1, n, h_wait, 0)
    h = jnp.sum(h_recv[...], axis=0) * scale
    gain = weights_ref[...] * jnp.sqrt(1.0 + h)
    new = n_sens * gain / jnp.sum(gain, axis=1, keepdims=True)
    new_ref[...] = new
    owned = jnp.sum(select * h, axis=1, keepdims=True)
    small = lax.broadcasted_iota(jnp.int32, (spd, spd), 0) == lax.broadcasted_iota(
        jnp.int32, (spd, spd), 1
    )
    owned_ref[...] = jnp.sum(jnp.where(small, owned, 0.0), axis=0, keepdims=True)
    lookup = ids_col == (lax.broadcasted_iota(jnp.int32, (nblk, n_sens), 1) + 1).astype(F32)
    factor = jnp.sum(jnp.where(lookup, new, 0.0), axis=1, keepdims=True)
    total = factor[0:1] * planes_ref[0]
    for j in range(1, nblk):
        total = total + factor[j : j + 1] * planes_ref[j]
    density_ref[...] = total

    def h_drain(k, carry):
        h_copy(k).wait_send()
        return carry

    lax.fori_loop(1, n, h_drain, 0)


def local(n_gx, n_gy, probes, blk_rows, blk_sensor, blk_count, coef, owner, weights):
    tile_r, tile_c, probe_n = probes.shape
    nblk, foot = blk_rows.shape
    n_sens = owner.shape[0]
    n = n_gx * n_gy
    width = LANES
    items = (foot // n_gx // 2) * (probe_n // width)
    tail = items // 6
    wide = max(LANES, nblk)
    batch = min(n_gx, max(1, 256 // nblk))

    vmem = pl.BlockSpec(memory_space=pltpu.VMEM)
    hbm = pl.BlockSpec(memory_space=pltpu.HBM)
    dma = pltpu.SemaphoreType.DMA
    owned, new, density = pl.pallas_call(
        functools.partial(step_kernel, n_gx, n_gy, 1.0 / (foot * probe_n), tail),
        out_shape=(
            jax.ShapeDtypeStruct((1, n_sens // n), F32),
            jax.ShapeDtypeStruct((1, n_sens), F32),
            jax.ShapeDtypeStruct((tile_r, tile_c), F32),
        ),
        in_specs=[hbm, hbm] + [vmem] * 6,
        out_specs=(vmem, vmem, vmem),
        scratch_shapes=[
            pltpu.SMEM((nblk, foot), jnp.int32),
            pltpu.VMEM((tile_r, tile_c, probe_n), BF16),
            pltpu.VMEM((tile_r * tile_c, probe_n), F32),
            pltpu.VMEM((batch, nblk, probe_n), F32),
            pltpu.VMEM((nblk, foot), F32),
            pltpu.VMEM((2, items, n_gx, nblk, width), BF16),
            pltpu.VMEM((2, items, n_gx, nblk, width), BF16),
            pltpu.VMEM((1, wide), F32),
            pltpu.VMEM((n_gx, 1, wide), F32),
            pltpu.VMEM((n_sens, n_gx * nblk), BF16),
            pltpu.VMEM((n_sens, width), F32),
            pltpu.VMEM((2, items, n_sens, width), BF16),
            pltpu.VMEM((2, items, n_sens, width), BF16),
            pltpu.VMEM((2, max(1, tail), n_sens, width), BF16),
            pltpu.VMEM((n_sens, LANES), F32),
            pltpu.VMEM((nblk, tile_r, tile_c), F32),
            pltpu.VMEM((1, n_sens), F32),
            pltpu.VMEM((n, 1, n_sens), F32),
            dma, dma((4,)), dma((2, items)), dma((2, items)), dma((n_gx,)), dma((n_gx,)),
            dma((2, items)), dma((2, items)), dma((2, max(1, tail))), dma((n,)), dma((n,)),
        ],
        compiler_params=pltpu.CompilerParams(
            collective_id=0, has_side_effects=True, vmem_limit_bytes=60 * 2**20
        ),
        name="reweight_step",
    )(
        blk_rows, probes, blk_count.reshape(1, 1), blk_sensor.reshape(1, nblk), blk_rows, coef,
        owner.reshape(1, n_sens), weights.reshape(1, n_sens),
    )
    return owned.reshape(-1), new.reshape(-1), density


def solution(mesh):
    n_gx, n_gy = mesh.shape["gx"], mesh.shape["gy"]
    in_specs = (
        P("gx", "gy", None),
        P(("gx", "gy"), None),
        P(("gx", "gy")),
        P(("gx", "gy")),
        P(("gx", "gy"), None),
        P(),
        P(),
    )
    out_specs = (P(("gx", "gy")), P(), P("gx", "gy"))
    return jax.shard_map(
        functools.partial(local, n_gx, n_gy),
        mesh=mesh, in_specs=in_specs, out_specs=out_specs, check_vma=False,
    )
```

```python
import functools

import jax
import jax.numpy as jnp
from jax import lax
from jax.experimental import pallas as pl
from jax.experimental.pallas import tpu as pltpu
from jax.sharding import PartitionSpec as P

MESH = pl.DeviceIdType.MESH
F32 = jnp.float32
BF16 = jnp.bfloat16
NT = (((1,), (1,)), ((), ()))
LANES = 128
LAG = 3
STACK = 1
TAIL = 4
AHEAD = 6
FRONT = 0


def step_kernel(
    n_gx, n_gy, scale, tail,
    rows_hbm, probes_hbm, count_hbm, sensor_hbm, coef_hbm, owner_hbm, weights_hbm,
    owned_hbm, new_hbm, density_hbm,
    count_ref, sensor_ref, rows_ref, coef_ref, owner_ref, weights_ref,
    owned_ref, new_ref, density_ref, small_sem, out_sem,
    rows_sm, probes_ref, tile_ref, stage_ref, coef32_ref, send_ref, recv_ref, ids_send, ids_recv,
    mixer_ref, own_ref, part_out, part_in, part_x, acc_ref, planes_ref, h_send, h_recv,
    rows_sem, load_sem, send_sem, recv_sem, ids_send_sem, ids_recv_sem, part_send_sem,
    part_sem, part_x_sem, h_send_sem, h_recv_sem,
):
    n = n_gx * n_gy
    gx = lax.axis_index("gx")
    gy = lax.axis_index("gy")
    flat = gx * n_gy + gy
    groups, _, nblk, probe_n = send_ref.shape[1:]
    items, part_rows, width = part_in.shape[1:]
    tile_r, tile_c = probes_ref.shape[:2]
    split = probe_n // width
    stack = owner_ref.shape[1] // part_rows
    fine = split * stack
    depth_k = n_gx * nblk
    n_sens = owner_ref.shape[1]
    foot = coef_ref.shape[1]
    wide = ids_send.shape[1]
    share = wide // nblk
    first_tail = items - tail

    parts = load_sem.shape[0]
    span = tile_r // parts

    def load(q):
        at = pl.ds(q * span, span)
        return pltpu.make_async_copy(probes_hbm.at[at], probes_ref.at[at], load_sem.at[q])

    pairs = (
        (count_hbm, count_ref), (sensor_hbm, sensor_ref), (rows_hbm, rows_ref),
        (coef_hbm, coef_ref), (owner_hbm, owner_ref), (weights_hbm, weights_ref),
    )
    small = [
        pltpu.make_async_copy(src, dst, small_sem.at[i]) for i, (src, dst) in enumerate(pairs)
    ]
    for copy in small:
        copy.start()
    for q in range(parts):
        load(q).start()
    rows_copy = pltpu.make_async_copy(rows_hbm, rows_sm, rows_sem)
    rows_copy.start()

    def across(j):
        return (lax.rem(gx + j, n_gx), gy)

    barrier = pltpu.get_barrier_semaphore()

    def greet(j, carry):
        pl.semaphore_signal(barrier, inc=1, device_id=across(j), device_id_type=MESH)
        return carry

    lax.fori_loop(1, n_gx, greet, 0)

    @pl.when(gy > 0)
    def _():
        pl.semaphore_signal(barrier, inc=1, device_id=(gx, gy - 1), device_id_type=MESH)

    @pl.when(gy < n_gy - 1)
    def _():
        pl.semaphore_signal(barrier, inc=1, device_id=(gx, gy + 1), device_id_type=MESH)

    for q in range(parts):
        load(q).wait()

        def widen(i, carry):
            rows = probes_ref[i].astype(F32)
            for p in range(split):
                at = pl.ds(i * (tile_c * split) + p, tile_c, stride=split)
                tile_ref[at, :] = rows[:, p * width : (p + 1) * width]
            return carry

        lax.fori_loop(q * span, (q + 1) * span, widen, 0)
    for copy in small:
        copy.wait()
    coef32_ref[...] = coef_ref[...].astype(F32)
    slot = lax.broadcasted_iota(jnp.int32, (1, nblk), 1)
    ids_one = jnp.where(slot < count_ref[...], sensor_ref[...] + 1, 0).astype(F32)
    down = lax.broadcasted_iota(jnp.int32, (nblk, nblk), 0)
    ids_col = jnp.sum(
        jnp.where(down == lax.broadcasted_iota(jnp.int32, (nblk, nblk), 1), ids_one, 0.0),
        axis=1, keepdims=True,
    )
    offset = lax.rem(gx, share) * nblk
    ids_send[...] = jnp.sum(
        jnp.where(
            lax.broadcasted_iota(jnp.int32, (nblk, wide), 1)
            == lax.broadcasted_iota(jnp.int32, (nblk, wide), 0) + offset,
            ids_col, 0.0,
        ),
        axis=0, keepdims=True,
    )
    ids_recv[gx] = ids_send[...]

    def plane(j, carry):
        at = rows_ref[pl.ds(j, 1), :]
        c = coef32_ref[pl.ds(j, 1), :]
        square = c * c
        top = square.astype(BF16).astype(F32)
        high = at // tile_c
        low = at - high * tile_c
        here = high == lax.broadcasted_iota(jnp.int32, (tile_r, foot), 0)
        left = jnp.concatenate(
            [jnp.where(here, top, 0.0), jnp.where(here, square - top, 0.0)], axis=0
        ).astype(BF16)
        right = jnp.where(
            low == lax.broadcasted_iota(jnp.int32, (tile_c, foot), 0), 1.0, 0.0
        ).astype(BF16)
        both = lax.dot_general(left, right, NT, preferred_element_type=F32)
        planes_ref[j] = both[:tile_r] + both[tile_r:]
        return carry

    lax.fori_loop(0, FRONT, plane, 0)
    rows_copy.wait()

    def block_copy(q, g, j):
        return pltpu.make_async_remote_copy(
            src_ref=send_ref.at[q, g, across(j)[0]], dst_ref=recv_ref.at[q, g, gx],
            send_sem=send_sem, recv_sem=recv_sem.at[q, g],
            device_id=across(j), device_id_type=MESH,
        )

    def ids_copy(j):
        return pltpu.make_async_remote_copy(
            src_ref=ids_send, dst_ref=ids_recv.at[gx],
            send_sem=ids_send_sem, recv_sem=ids_recv_sem,
            device_id=across(j), device_id_type=MESH,
        )

    def part_copy(q, c, up):
        return pltpu.make_async_remote_copy(
            src_ref=part_out.at[q * items + c], dst_ref=part_in.at[q, c],
            send_sem=part_send_sem, recv_sem=part_sem.at[q, c],
            device_id=(gx, gy + up), device_id_type=MESH,
        )

    def part_x_copy(q, c, up):
        return pltpu.make_async_remote_copy(
            src_ref=part_out.at[q * items + c], dst_ref=part_x.at[q, c - first_tail],
            send_sem=part_send_sem, recv_sem=part_x_sem.at[q, c - first_tail],
            device_id=(gx, gy + up), device_id_type=MESH,
        )

    def h_peer(k):
        far = k // n_gx
        tz = jnp.where(gy < n_gy // 2, n_gy - 1 - far, far)
        tx = lax.rem(gx + lax.rem(k, n_gx), n_gx)
        return tx * n_gy + tz, (tx, tz)

    def h_copy(k):
        return pltpu.make_async_remote_copy(
            src_ref=h_send, dst_ref=h_recv.at[flat],
            send_sem=h_send_sem, recv_sem=h_recv_sem,
            device_id=h_peer(k)[1], device_id_type=MESH,
        )

    channel = lax.broadcasted_iota(jnp.int32, (nblk, foot), 1)
    batch = stage_ref.shape[0]

    def gather(q, g):
        def some(b, carry):
            for e in range(batch):
                d = b * batch + e
                r = (g * 2 + q) * n_gx + d
                column = jnp.sum(
                    jnp.where(channel == r, coef32_ref[...], 0.0), axis=1, keepdims=True
                )
                for j in range(nblk):
                    at = rows_sm[j, r] * split
                    stage_ref[e, pl.ds(j * split, split), :] = tile_ref[pl.ds(at, split), :]
                for p in range(split):
                    part = stage_ref[e, pl.ds(p, nblk, stride=split), :]
                    send_ref[q, g, d, :, p * width : (p + 1) * width] = (part * column).astype(BF16)
            return carry

        lax.fori_loop(0, n_gx // batch, some, 0)

    def launch(q, g):
        recv_ref[q, g, gx] = send_ref[q, g, gx]
        for j in range(1, n_gx):
            block_copy(q, g, j).start()

    gather(0, 0)
    pl.semaphore_wait(
        barrier,
        n_gx - 1 + jnp.where(gy > 0, 1, 0) + jnp.where(gy < n_gy - 1, 1, 0),
    )
    for j in range(1, n_gx):
        ids_copy(j).start()
    launch(0, 0)

    def gather_on(k, carry):
        gather(k % 2, k // 2)
        launch(k % 2, k // 2)
        return carry

    lax.fori_loop(1, AHEAD, gather_on, 0)

    rest = pl.ds(0, n_gx - 1)
    pltpu.make_async_copy(ids_recv.at[rest], ids_recv.at[rest], ids_recv_sem).wait()
    sensor_up = (lax.broadcasted_iota(jnp.int32, (n_sens, wide), 0) + 1).astype(F32)
    for piece in range(n_gx // share):
        row = ids_recv[piece * share]
        for extra in range(1, share):
            row = row + ids_recv[piece * share + extra]
        mixer_ref[:, piece * wide : (piece + 1) * wide] = jnp.where(
            row == sensor_up, 1.0, 0.0
        ).astype(BF16)
    acc_ref[...] = jnp.zeros_like(acc_ref)

    others = pl.ds(0, n_gx - 1)

    def mix(q, g):
        pltpu.make_async_copy(
            send_ref.at[q, g, others], recv_ref.at[q, g, others], recv_sem.at[q, g]
        ).wait()
        y = jnp.dot(
            mixer_ref[...], recv_ref[q, g].reshape(depth_k, probe_n), preferred_element_type=F32
        )
        for p in range(split):
            for v in range(stack):
                own_ref[q, (g * split + p) * stack + v] = y[
                    v * part_rows : (v + 1) * part_rows, p * width : (p + 1) * width
                ]

    def collect(q, c, f, crossing):
        below = (gy > 0) & (gy <= f)
        above = (gy < n_gy - 1) & (gy >= f)

        @pl.when(below if q == 0 else above)
        def _():
            pltpu.make_async_copy(part_out.at[0], part_in.at[q, c], part_sem.at[q, c]).wait()
            own_ref[q, c] += part_in[q, c].astype(F32)

        if crossing:
            @pl.when(above if q == 0 else below)
            def _():
                at = c - first_tail
                pltpu.make_async_copy(
                    part_out.at[0], part_x.at[q, at], part_x_sem.at[q, at]
                ).wait()
                own_ref[q, c] += part_x[q, at].astype(F32)

        @pl.when(gy == f)
        def _():
            v = lax.rem(c, stack)
            total = acc_ref[v]
            for at in range(0, width, LANES):
                y = own_ref[q, c, :, at : at + LANES]
                total = total + y * y
            acc_ref[v] = total

    def process(q, c, f, crossing, head):
        if not head:
            collect(q, c, f, crossing)

        @pl.when(gy < f)
        def _():
            part_out[q * items + c] = own_ref[q, c].astype(BF16)
            (part_copy if q == 0 else part_x_copy)(q, c, 1).start()

        @pl.when(gy > f)
        def _():
            part_out[q * items + c] = own_ref[q, c].astype(BF16)
            (part_copy if q == 1 else part_x_copy)(q, c, -1).start()

    def ends(q, crossing):
        if crossing:
            return n_gy // 2 - q
        return n_gy - 1 if q == 0 else 0

    def depth_of(f):
        low = jnp.where(gy <= f, gy, 0)
        high = jnp.where(gy >= f, n_gy - 1 - gy, 0)
        return jnp.maximum(low, high)

    late = fine // 2
    every, halves = max(1, fine // 2), max(1, 2 // fine)
    each = max(0, nblk - FRONT) // (2 * AHEAD)
    steps = items + late + LAG * (n_gy - 1)

    def turns(s, q, crossing):
        f = ends(q, crossing)
        lo, hi = (first_tail, items) if crossing else (0, first_tail)
        depth = depth_of(f)
        c = s - LAG * depth - (late if q else 0)
        return f, depth, c, (c >= lo) & (c < hi)

    kinds = (True, False) if tail else (False,)

    def chain(s):
        for crossing in kinds:
            for q in range(2):
                f, depth, c, turn = turns(s, q, crossing)

                @pl.when(turn & (depth > 0))
                def _():
                    process(q, c, f, crossing, False)

    def heads(s):
        for crossing in reversed(kinds):
            for q in range(2):
                f, depth, c, turn = turns(s, q, crossing)

                @pl.when(turn & (depth == 0) & ((gy == 0) if q == 0 else (gy > 0)))
                def _():
                    process(q, c, f, crossing, True)
        if tail:
            for q in range(2):
                f, depth, c, turn = turns(s - tail, q, True)

                @pl.when(turn & (depth == 0) & ((gy > 0) if q == 0 else (gy == 0)))
                def _():
                    process(q, c, f, True, True)

    def step(s, carry):
        chain(s)
        for e in range(halves):
            k = s // every * halves + e
            turn = lax.rem(s, every) == 0

            @pl.when(turn & (k + AHEAD < 2 * groups))
            def _():
                gather((k + AHEAD) % 2, (k + AHEAD) // 2)
                launch((k + AHEAD) % 2, (k + AHEAD) // 2)

            @pl.when(turn & (k + AHEAD >= 2 * groups) & (k < 2 * groups))
            def _():
                for b in range(each):
                    plane(FRONT + (k + AHEAD - 2 * groups) * each + b, 0)

            @pl.when(turn & (k < 2 * groups))
            def _():
                mix(k % 2, k // 2)

        heads(s)
        return carry

    lax.fori_loop(0, steps, step, 0)

    h_send[...] = lax.dot_general(
        jnp.ones((8, LANES), F32), acc_ref[...].reshape(n_sens, LANES), NT,
        precision=lax.Precision.HIGHEST, preferred_element_type=F32,
    )[0:1]
    h_recv[flat] = h_send[...]

    def h_launch(k, carry):
        @pl.when(h_peer(k)[0] != flat)
        def _():
            h_copy(k).start()
        return carry

    lax.fori_loop(0, n, h_launch, 0)
    lax.fori_loop(FRONT + AHEAD * each, nblk, plane, 0)

    spd = n_sens // n
    mine = jnp.where(owner_ref[...] == flat, 1.0, 0.0)
    before = jnp.where(
        lax.broadcasted_iota(jnp.int32, (n_sens, n_sens), 0)
        < lax.broadcasted_iota(jnp.int32, (n_sens, n_sens), 1),
        1.0, 0.0,
    ).astype(BF16)
    rank = jnp.dot(
        jnp.broadcast_to(mine, (spd, n_sens)).astype(BF16), before, preferred_element_type=F32
    )
    place = lax.broadcasted_iota(jnp.int32, (spd, n_sens), 0).astype(F32)
    select = jnp.where(rank == place, 1.0, 0.0) * mine

    def drain(count):
        sent = pl.ds(0, 2 * items - count)
        pltpu.make_async_copy(part_out.at[sent], part_out.at[sent], part_send_sem).wait()

    middle = (gy == n_gy // 2) | (gy == n_gy // 2 - 1)
    edge = (gy == 0) | (gy == n_gy - 1)
    pl.when(edge)(lambda: drain(first_tail))
    pl.when(middle & jnp.logical_not(edge))(lambda: drain(tail))
    pl.when(jnp.logical_not(middle | edge))(lambda: drain(0))
    whole = pl.ds(0, n_gx - 1)
    pltpu.make_async_copy(
        send_ref.at[:, :, whole], recv_ref.at[:, :, whole], send_sem
    ).wait()
    pltpu.make_async_copy(ids_recv.at[rest], ids_recv.at[rest], ids_send_sem).wait()

    peers = h_recv.at[pl.ds(0, n - 1)]
    pltpu.make_async_copy(peers, peers, h_send_sem).wait()
    pltpu.make_async_copy(peers, peers, h_recv_sem).wait()
    h = jnp.sum(h_recv[...], axis=0) * scale
    gain = weights_ref[...] * jnp.sqrt(1.0 + h)
    new = n_sens * gain / jnp.sum(gain, axis=1, keepdims=True)
    new_ref[...] = new
    owned = jnp.sum(select * h, axis=1, keepdims=True)
    small = lax.broadcasted_iota(jnp.int32, (spd, spd), 0) == lax.broadcasted_iota(
        jnp.int32, (spd, spd), 1
    )
    owned_ref[...] = jnp.sum(jnp.where(small, owned, 0.0), axis=0, keepdims=True)
    lookup = ids_col == (lax.broadcasted_iota(jnp.int32, (nblk, n_sens), 1) + 1).astype(F32)
    factor = jnp.sum(jnp.where(lookup, new, 0.0), axis=1, keepdims=True)
    total = factor[0:1] * planes_ref[0]
    for j in range(1, nblk):
        total = total + factor[j : j + 1] * planes_ref[j]
    density_ref[...] = total
    results = (
        (owned_ref, owned_hbm), (new_ref, new_hbm), (density_ref, density_hbm),
    )
    out = [pltpu.make_async_copy(src, dst, out_sem.at[i]) for i, (src, dst) in enumerate(results)]
    for copy in out:
        copy.start()
    for copy in out:
        copy.wait()


def write_kernel(owned_in, new_in, density_in, owned_ref, new_ref, density_ref):
    owned_ref[...] = owned_in[...]
    new_ref[...] = new_in[...]
    density_ref[...] = density_in[...]


def local(n_gx, n_gy, probes, blk_rows, blk_sensor, blk_count, coef, owner, weights):
    tile_r, tile_c, probe_n = probes.shape
    nblk, foot = blk_rows.shape
    n_sens = owner.shape[0]
    n = n_gx * n_gy
    width = LANES
    groups, split = foot // n_gx // 2, probe_n // width
    stack = STACK
    part_rows = n_sens // stack
    items = groups * split * stack
    tail = TAIL * items // 32 if n_gy > 3 else 0
    wide = max(LANES, nblk)
    batch = min(n_gx, max(1, 256 // nblk))

    vmem = pl.BlockSpec(memory_space=pltpu.VMEM)
    hbm = pl.BlockSpec(memory_space=pltpu.HBM)
    dma = pltpu.SemaphoreType.DMA
    outs = (
        jax.ShapeDtypeStruct((1, n_sens // n), F32),
        jax.ShapeDtypeStruct((1, n_sens), F32),
        jax.ShapeDtypeStruct((tile_r, tile_c), F32),
    )
    results = pl.pallas_call(
        functools.partial(step_kernel, n_gx, n_gy, 1.0 / (foot * probe_n), tail),
        out_shape=outs,
        in_specs=[hbm] * 7,
        out_specs=(hbm, hbm, hbm),
        scratch_shapes=[
            pltpu.VMEM((1, 1), jnp.int32),
            pltpu.VMEM((1, nblk), jnp.int32),
            pltpu.VMEM((nblk, foot), jnp.int32),
            pltpu.VMEM((nblk, foot), BF16),
            pltpu.VMEM((1, n_sens), jnp.int32),
            pltpu.VMEM((1, n_sens), F32),
            pltpu.VMEM((1, n_sens // n), F32),
            pltpu.VMEM((1, n_sens), F32),
            pltpu.VMEM((tile_r, tile_c), F32),
            dma((6,)), dma((3,)),
            pltpu.SMEM((nblk, foot), jnp.int32),
            pltpu.VMEM((tile_r, tile_c, probe_n), BF16),
            pltpu.VMEM((tile_r * tile_c * split, width), F32),
            pltpu.VMEM((batch, nblk * split, width), F32),
            pltpu.VMEM((nblk, foot), F32),
            pltpu.VMEM((2, groups, n_gx, nblk, probe_n), BF16),
            pltpu.VMEM((2, groups, n_gx, nblk, probe_n), BF16),
            pltpu.VMEM((1, wide), F32),
            pltpu.VMEM((n_gx, 1, wide), F32),
            pltpu.VMEM((n_sens, n_gx * nblk), BF16),
            pltpu.VMEM((2, items, part_rows, width), F32),
            pltpu.VMEM((2 * items, part_rows, width), BF16),
            pltpu.VMEM((2, items, part_rows, width), BF16),
            pltpu.VMEM((2, max(1, tail), part_rows, width), BF16),
            pltpu.VMEM((stack, part_rows, LANES), F32),
            pltpu.VMEM((nblk, tile_r, tile_c), F32),
            pltpu.VMEM((1, n_sens), F32),
            pltpu.VMEM((n, 1, n_sens), F32),
            dma, dma((4,)), dma, dma((2, groups)), dma, dma, dma,
            dma((2, items)), dma((2, max(1, tail))), dma, dma,
        ],
        compiler_params=pltpu.CompilerParams(
            collective_id=0, has_side_effects=True, vmem_limit_bytes=60 * 2**20
        ),
        name="reweight_step",
    )(
        blk_rows, probes, blk_count.reshape(1, 1), blk_sensor.reshape(1, nblk), coef,
        owner.reshape(1, n_sens), weights.reshape(1, n_sens),
    )
    owned, new, density = pl.pallas_call(
        write_kernel,
        out_shape=outs,
        in_specs=[vmem] * 3,
        out_specs=(vmem,) * 3,
        name="write_results",
    )(*results)
    return owned.reshape(-1), new.reshape(-1), density


def solution(mesh):
    n_gx, n_gy = mesh.shape["gx"], mesh.shape["gy"]
    in_specs = (
        P("gx", "gy", None),
        P(("gx", "gy"), None),
        P(("gx", "gy")),
        P(("gx", "gy")),
        P(("gx", "gy"), None),
        P(),
        P(),
    )
    out_specs = (P(("gx", "gy")), P(), P("gx", "gy"))
    return jax.shard_map(
        functools.partial(local, n_gx, n_gy),
        mesh=mesh, in_specs=in_specs, out_specs=out_specs, check_vma=False,
    )
```

```python
import functools

import jax
import jax.numpy as jnp
from jax import lax
from jax.experimental import pallas as pl
from jax.experimental.pallas import tpu as pltpu
from jax.sharding import PartitionSpec as P

MESH = pl.DeviceIdType.MESH
F32 = jnp.float32
BF16 = jnp.bfloat16
NT = (((1,), (1,)), ((), ()))
LANES = 128
LAG = 3
STACK = 1
TAIL = 4
AHEAD = 6
FRONT = 0


def step_kernel(
    n_gx, n_gy, scale, tail,
    rows_hbm, probes_hbm, count_hbm, sensor_hbm, coef_hbm, owner_hbm, weights_hbm,
    owned_ref, new_ref, density_ref,
    count_ref, sensor_ref, rows_ref, coef_ref, owner_ref, weights_ref,
    small_sem,
    rows_sm, probes_ref, tile_ref, stage_ref, coef32_ref, send_ref, recv_ref, ids_send, ids_recv,
    mixer_ref, own_ref, part_out, part_in, part_x, acc_ref, planes_ref, h_send, h_recv,
    rows_sem, load_sem, send_sem, recv_sem, ids_send_sem, ids_recv_sem, part_send_sem,
    part_sem, part_x_sem, h_send_sem, h_recv_sem,
):
    n = n_gx * n_gy
    gx = lax.axis_index("gx")
    gy = lax.axis_index("gy")
    flat = gx * n_gy + gy
    groups, _, nblk, probe_n = send_ref.shape[1:]
    items, part_rows, width = part_in.shape[1:]
    tile_r, tile_c = probes_ref.shape[:2]
    split = probe_n // width
    stack = owner_ref.shape[1] // part_rows
    fine = split * stack
    depth_k = n_gx * nblk
    n_sens = owner_ref.shape[1]
    foot = coef_ref.shape[1]
    wide = ids_send.shape[1]
    share = wide // nblk
    first_tail = items - tail

    parts = load_sem.shape[0]
    span = tile_r // parts

    def load(q):
        at = pl.ds(q * span, span)
        return pltpu.make_async_copy(probes_hbm.at[at], probes_ref.at[at], load_sem.at[q])

    pairs = (
        (count_hbm, count_ref), (sensor_hbm, sensor_ref), (rows_hbm, rows_ref),
        (coef_hbm, coef_ref), (owner_hbm, owner_ref), (weights_hbm, weights_ref),
    )
    small = [
        pltpu.make_async_copy(src, dst, small_sem.at[i]) for i, (src, dst) in enumerate(pairs)
    ]
    for copy in small:
        copy.start()
    for q in range(parts):
        load(q).start()
    rows_copy = pltpu.make_async_copy(rows_hbm, rows_sm, rows_sem)
    rows_copy.start()

    def across(j):
        return (lax.rem(gx + j, n_gx), gy)

    barrier = pltpu.get_barrier_semaphore()

    def greet(j, carry):
        pl.semaphore_signal(barrier, inc=1, device_id=across(j), device_id_type=MESH)
        return carry

    lax.fori_loop(1, n_gx, greet, 0)

    @pl.when(gy > 0)
    def _():
        pl.semaphore_signal(barrier, inc=1, device_id=(gx, gy - 1), device_id_type=MESH)

    @pl.when(gy < n_gy - 1)
    def _():
        pl.semaphore_signal(barrier, inc=1, device_id=(gx, gy + 1), device_id_type=MESH)

    for q in range(parts):
        load(q).wait()

        def widen(i, carry):
            rows = probes_ref[i].astype(F32)
            for p in range(split):
                at = pl.ds(i * (tile_c * split) + p, tile_c, stride=split)
                tile_ref[at, :] = rows[:, p * width : (p + 1) * width]
            return carry

        lax.fori_loop(q * span, (q + 1) * span, widen, 0)
    for copy in small:
        copy.wait()
    coef32_ref[...] = coef_ref[...].astype(F32)
    slot = lax.broadcasted_iota(jnp.int32, (1, nblk), 1)
    ids_one = jnp.where(slot < count_ref[...], sensor_ref[...] + 1, 0).astype(F32)
    down = lax.broadcasted_iota(jnp.int32, (nblk, nblk), 0)
    ids_col = jnp.sum(
        jnp.where(down == lax.broadcasted_iota(jnp.int32, (nblk, nblk), 1), ids_one, 0.0),
        axis=1, keepdims=True,
    )
    offset = lax.rem(gx, share) * nblk
    ids_send[...] = jnp.sum(
        jnp.where(
            lax.broadcasted_iota(jnp.int32, (nblk, wide), 1)
            == lax.broadcasted_iota(jnp.int32, (nblk, wide), 0) + offset,
            ids_col, 0.0,
        ),
        axis=0, keepdims=True,
    )
    ids_recv[gx] = ids_send[...]

    def plane(j, carry):
        at = rows_ref[pl.ds(j, 1), :]
        c = coef32_ref[pl.ds(j, 1), :]
        square = c * c
        top = square.astype(BF16).astype(F32)
        high = at // tile_c
        low = at - high * tile_c
        here = high == lax.broadcasted_iota(jnp.int32, (tile_r, foot), 0)
        left = jnp.concatenate(
            [jnp.where(here, top, 0.0), jnp.where(here, square - top, 0.0)], axis=0
        ).astype(BF16)
        right = jnp.where(
            low == lax.broadcasted_iota(jnp.int32, (tile_c, foot), 0), 1.0, 0.0
        ).astype(BF16)
        both = lax.dot_general(left, right, NT, preferred_element_type=F32)
        planes_ref[j] = both[:tile_r] + both[tile_r:]
        return carry

    lax.fori_loop(0, FRONT, plane, 0)
    rows_copy.wait()

    def block_copy(q, g, j):
        return pltpu.make_async_remote_copy(
            src_ref=send_ref.at[q, g, across(j)[0]], dst_ref=recv_ref.at[q, g, gx],
            send_sem=send_sem, recv_sem=recv_sem.at[q, g],
            device_id=across(j), device_id_type=MESH,
        )

    def ids_copy(j):
        return pltpu.make_async_remote_copy(
            src_ref=ids_send, dst_ref=ids_recv.at[gx],
            send_sem=ids_send_sem, recv_sem=ids_recv_sem,
            device_id=across(j), device_id_type=MESH,
        )

    def part_copy(q, c, up):
        return pltpu.make_async_remote_copy(
            src_ref=part_out.at[q * items + c], dst_ref=part_in.at[q, c],
            send_sem=part_send_sem, recv_sem=part_sem.at[q, c],
            device_id=(gx, gy + up), device_id_type=MESH,
        )

    def part_x_copy(q, c, up):
        return pltpu.make_async_remote_copy(
            src_ref=part_out.at[q * items + c], dst_ref=part_x.at[q, c - first_tail],
            send_sem=part_send_sem, recv_sem=part_x_sem.at[q, c - first_tail],
            device_id=(gx, gy + up), device_id_type=MESH,
        )

    def h_peer(k):
        far = k // n_gx
        tz = jnp.where(gy < n_gy // 2, n_gy - 1 - far, far)
        tx = lax.rem(gx + lax.rem(k, n_gx), n_gx)
        return tx * n_gy + tz, (tx, tz)

    def h_copy(k):
        return pltpu.make_async_remote_copy(
            src_ref=h_send, dst_ref=h_recv.at[flat],
            send_sem=h_send_sem, recv_sem=h_recv_sem,
            device_id=h_peer(k)[1], device_id_type=MESH,
        )

    channel = lax.broadcasted_iota(jnp.int32, (nblk, foot), 1)
    batch = stage_ref.shape[0]

    def gather(q, g):
        def some(b, carry):
            for e in range(batch):
                d = b * batch + e
                r = (g * 2 + q) * n_gx + d
                column = jnp.sum(
                    jnp.where(channel == r, coef32_ref[...], 0.0), axis=1, keepdims=True
                )
                for j in range(nblk):
                    at = rows_sm[j, r] * split
                    stage_ref[e, pl.ds(j * split, split), :] = tile_ref[pl.ds(at, split), :]
                for p in range(split):
                    part = stage_ref[e, pl.ds(p, nblk, stride=split), :]
                    send_ref[q, g, d, :, p * width : (p + 1) * width] = (part * column).astype(BF16)
            return carry

        lax.fori_loop(0, n_gx // batch, some, 0)

    def launch(q, g):
        recv_ref[q, g, gx] = send_ref[q, g, gx]
        for j in range(1, n_gx):
            block_copy(q, g, j).start()

    gather(0, 0)
    pl.semaphore_wait(
        barrier,
        n_gx - 1 + jnp.where(gy > 0, 1, 0) + jnp.where(gy < n_gy - 1, 1, 0),
    )
    for j in range(1, n_gx):
        ids_copy(j).start()
    launch(0, 0)

    def gather_on(k, carry):
        gather(k % 2, k // 2)
        launch(k % 2, k // 2)
        return carry

    lax.fori_loop(1, AHEAD, gather_on, 0)

    rest = pl.ds(0, n_gx - 1)
    pltpu.make_async_copy(ids_recv.at[rest], ids_recv.at[rest], ids_recv_sem).wait()
    sensor_up = (lax.broadcasted_iota(jnp.int32, (n_sens, wide), 0) + 1).astype(F32)
    for piece in range(n_gx // share):
        row = ids_recv[piece * share]
        for extra in range(1, share):
            row = row + ids_recv[piece * share + extra]
        mixer_ref[:, piece * wide : (piece + 1) * wide] = jnp.where(
            row == sensor_up, 1.0, 0.0
        ).astype(BF16)
    acc_ref[...] = jnp.zeros_like(acc_ref)

    others = pl.ds(0, n_gx - 1)

    def mix(q, g):
        pltpu.make_async_copy(
            send_ref.at[q, g, others], recv_ref.at[q, g, others], recv_sem.at[q, g]
        ).wait()
        y = jnp.dot(
            mixer_ref[...], recv_ref[q, g].reshape(depth_k, probe_n), preferred_element_type=F32
        )
        for p in range(split):
            for v in range(stack):
                own_ref[q, (g * split + p) * stack + v] = y[
                    v * part_rows : (v + 1) * part_rows, p * width : (p + 1) * width
                ]

    def collect(q, c, f, crossing):
        below = (gy > 0) & (gy <= f)
        above = (gy < n_gy - 1) & (gy >= f)

        @pl.when(below if q == 0 else above)
        def _():
            pltpu.make_async_copy(part_out.at[0], part_in.at[q, c], part_sem.at[q, c]).wait()
            own_ref[q, c] += part_in[q, c].astype(F32)

        if crossing:
            @pl.when(above if q == 0 else below)
            def _():
                at = c - first_tail
                pltpu.make_async_copy(
                    part_out.at[0], part_x.at[q, at], part_x_sem.at[q, at]
                ).wait()
                own_ref[q, c] += part_x[q, at].astype(F32)

        @pl.when(gy == f)
        def _():
            v = lax.rem(c, stack)
            total = acc_ref[v]
            for at in range(0, width, LANES):
                y = own_ref[q, c, :, at : at + LANES]
                total = total + y * y
            acc_ref[v] = total

    def process(q, c, f, crossing, head):
        if not head:
            collect(q, c, f, crossing)

        @pl.when(gy < f)
        def _():
            part_out[q * items + c] = own_ref[q, c].astype(BF16)
            (part_copy if q == 0 else part_x_copy)(q, c, 1).start()

        @pl.when(gy > f)
        def _():
            part_out[q * items + c] = own_ref[q, c].astype(BF16)
            (part_copy if q == 1 else part_x_copy)(q, c, -1).start()

    def ends(q, crossing):
        if crossing:
            return n_gy // 2 - q
        return n_gy - 1 if q == 0 else 0

    def depth_of(f):
        low = jnp.where(gy <= f, gy, 0)
        high = jnp.where(gy >= f, n_gy - 1 - gy, 0)
        return jnp.maximum(low, high)

    late = fine // 2
    every, halves = max(1, fine // 2), max(1, 2 // fine)
    each = max(0, nblk - FRONT) // (2 * AHEAD)
    steps = items + late + LAG * (n_gy - 1)

    def turns(s, q, crossing):
        f = ends(q, crossing)
        lo, hi = (first_tail, items) if crossing else (0, first_tail)
        depth = depth_of(f)
        c = s - LAG * depth - (late if q else 0)
        return f, depth, c, (c >= lo) & (c < hi)

    kinds = (True, False) if tail else (False,)

    def chain(s):
        for crossing in kinds:
            for q in range(2):
                f, depth, c, turn = turns(s, q, crossing)

                @pl.when(turn & (depth > 0))
                def _():
                    process(q, c, f, crossing, False)

    def heads(s):
        for crossing in reversed(kinds):
            for q in range(2):
                f, depth, c, turn = turns(s, q, crossing)

                @pl.when(turn & (depth == 0) & ((gy == 0) if q == 0 else (gy > 0)))
                def _():
                    process(q, c, f, crossing, True)
        if tail:
            for q in range(2):
                f, depth, c, turn = turns(s - tail, q, True)

                @pl.when(turn & (depth == 0) & ((gy > 0) if q == 0 else (gy == 0)))
                def _():
                    process(q, c, f, True, True)

    def step(s, carry):
        chain(s)
        for e in range(halves):
            k = s // every * halves + e
            turn = lax.rem(s, every) == 0

            @pl.when(turn & (k + AHEAD < 2 * groups))
            def _():
                gather((k + AHEAD) % 2, (k + AHEAD) // 2)
                launch((k + AHEAD) % 2, (k + AHEAD) // 2)

            @pl.when(turn & (k + AHEAD >= 2 * groups) & (k < 2 * groups))
            def _():
                for b in range(each):
                    plane(FRONT + (k + AHEAD - 2 * groups) * each + b, 0)

            @pl.when(turn & (k < 2 * groups))
            def _():
                mix(k % 2, k // 2)

        heads(s)
        return carry

    lax.fori_loop(0, steps, step, 0)

    h_send[...] = lax.dot_general(
        jnp.ones((8, LANES), F32), acc_ref[...].reshape(n_sens, LANES), NT,
        precision=lax.Precision.HIGHEST, preferred_element_type=F32,
    )[0:1]
    h_recv[flat] = h_send[...]

    def h_launch(k, carry):
        @pl.when(h_peer(k)[0] != flat)
        def _():
            h_copy(k).start()
        return carry

    lax.fori_loop(0, n, h_launch, 0)
    lax.fori_loop(FRONT + AHEAD * each, nblk, plane, 0)

    spd = n_sens // n
    mine = jnp.where(owner_ref[...] == flat, 1.0, 0.0)
    before = jnp.where(
        lax.broadcasted_iota(jnp.int32, (n_sens, n_sens), 0)
        < lax.broadcasted_iota(jnp.int32, (n_sens, n_sens), 1),
        1.0, 0.0,
    ).astype(BF16)
    rank = jnp.dot(
        jnp.broadcast_to(mine, (spd, n_sens)).astype(BF16), before, preferred_element_type=F32
    )
    place = lax.broadcasted_iota(jnp.int32, (spd, n_sens), 0).astype(F32)
    select = jnp.where(rank == place, 1.0, 0.0) * mine

    def drain(count):
        sent = pl.ds(0, 2 * items - count)
        pltpu.make_async_copy(part_out.at[sent], part_out.at[sent], part_send_sem).wait()

    middle = (gy == n_gy // 2) | (gy == n_gy // 2 - 1)
    edge = (gy == 0) | (gy == n_gy - 1)
    pl.when(edge)(lambda: drain(first_tail))
    pl.when(middle & jnp.logical_not(edge))(lambda: drain(tail))
    pl.when(jnp.logical_not(middle | edge))(lambda: drain(0))
    whole = pl.ds(0, n_gx - 1)
    pltpu.make_async_copy(
        send_ref.at[:, :, whole], recv_ref.at[:, :, whole], send_sem
    ).wait()
    pltpu.make_async_copy(ids_recv.at[rest], ids_recv.at[rest], ids_send_sem).wait()

    peers = h_recv.at[pl.ds(0, n - 1)]
    pltpu.make_async_copy(peers, peers, h_send_sem).wait()
    pltpu.make_async_copy(peers, peers, h_recv_sem).wait()
    h = jnp.sum(h_recv[...], axis=0) * scale
    gain = weights_ref[...] * jnp.sqrt(1.0 + h)
    new = n_sens * gain / jnp.sum(gain, axis=1, keepdims=True)
    new_ref[...] = new
    owned = jnp.sum(select * h, axis=1, keepdims=True)
    small = lax.broadcasted_iota(jnp.int32, (spd, spd), 0) == lax.broadcasted_iota(
        jnp.int32, (spd, spd), 1
    )
    owned_ref[...] = jnp.sum(jnp.where(small, owned, 0.0), axis=0, keepdims=True)
    lookup = ids_col == (lax.broadcasted_iota(jnp.int32, (nblk, n_sens), 1) + 1).astype(F32)
    factor = jnp.sum(jnp.where(lookup, new, 0.0), axis=1, keepdims=True)
    total = factor[0:1] * planes_ref[0]
    for j in range(1, nblk):
        total = total + factor[j : j + 1] * planes_ref[j]
    density_ref[...] = total


def write_kernel(owned_in, new_in, density_in, owned_ref, new_ref, density_ref):
    owned_ref[...] = owned_in[...]
    new_ref[...] = new_in[...]
    density_ref[...] = density_in[...]


def local(n_gx, n_gy, probes, blk_rows, blk_sensor, blk_count, coef, owner, weights):
    tile_r, tile_c, probe_n = probes.shape
    nblk, foot = blk_rows.shape
    n_sens = owner.shape[0]
    n = n_gx * n_gy
    width = LANES
    groups, split = foot // n_gx // 2, probe_n // width
    stack = STACK
    part_rows = n_sens // stack
    items = groups * split * stack
    tail = TAIL * items // 32 if n_gy > 3 else 0
    wide = max(LANES, nblk)
    batch = min(n_gx, max(1, 256 // nblk))

    vmem = pl.BlockSpec(memory_space=pltpu.VMEM)
    hbm = pl.BlockSpec(memory_space=pltpu.HBM)
    dma = pltpu.SemaphoreType.DMA
    outs = (
        jax.ShapeDtypeStruct((1, n_sens // n), F32),
        jax.ShapeDtypeStruct((1, n_sens), F32),
        jax.ShapeDtypeStruct((tile_r, tile_c), F32),
    )
    results = pl.pallas_call(
        functools.partial(step_kernel, n_gx, n_gy, 1.0 / (foot * probe_n), tail),
        out_shape=tuple(pltpu.VMEM(out.shape, out.dtype) for out in outs),
        in_specs=[hbm] * 7,
        out_specs=(vmem,) * 3,
        scratch_shapes=[
            pltpu.VMEM((1, 1), jnp.int32),
            pltpu.VMEM((1, nblk), jnp.int32),
            pltpu.VMEM((nblk, foot), jnp.int32),
            pltpu.VMEM((nblk, foot), BF16),
            pltpu.VMEM((1, n_sens), jnp.int32),
            pltpu.VMEM((1, n_sens), F32),
            dma((6,)),
            pltpu.SMEM((nblk, foot), jnp.int32),
            pltpu.VMEM((tile_r, tile_c, probe_n), BF16),
            pltpu.VMEM((tile_r * tile_c * split, width), F32),
            pltpu.VMEM((batch, nblk * split, width), F32),
            pltpu.VMEM((nblk, foot), F32),
            pltpu.VMEM((2, groups, n_gx, nblk, probe_n), BF16),
            pltpu.VMEM((2, groups, n_gx, nblk, probe_n), BF16),
            pltpu.VMEM((1, wide), F32),
            pltpu.VMEM((n_gx, 1, wide), F32),
            pltpu.VMEM((n_sens, n_gx * nblk), BF16),
            pltpu.VMEM((2, items, part_rows, width), F32),
            pltpu.VMEM((2 * items, part_rows, width), BF16),
            pltpu.VMEM((2, items, part_rows, width), BF16),
            pltpu.VMEM((2, max(1, tail), part_rows, width), BF16),
            pltpu.VMEM((stack, part_rows, LANES), F32),
            pltpu.VMEM((nblk, tile_r, tile_c), F32),
            pltpu.VMEM((1, n_sens), F32),
            pltpu.VMEM((n, 1, n_sens), F32),
            dma, dma((4,)), dma, dma((2, groups)), dma, dma, dma,
            dma((2, items)), dma((2, max(1, tail))), dma, dma,
        ],
        compiler_params=pltpu.CompilerParams(
            collective_id=0, has_side_effects=True, vmem_limit_bytes=60 * 2**20
        ),
        name="reweight_step",
    )(
        blk_rows, probes, blk_count.reshape(1, 1), blk_sensor.reshape(1, nblk), coef,
        owner.reshape(1, n_sens), weights.reshape(1, n_sens),
    )
    owned, new, density = pl.pallas_call(
        write_kernel,
        out_shape=outs,
        in_specs=[vmem] * 3,
        out_specs=(vmem,) * 3,
        name="write_results",
    )(*[pltpu.with_memory_space_constraint(r, pltpu.VMEM) for r in results])
    return owned.reshape(-1), new.reshape(-1), density


def solution(mesh):
    n_gx, n_gy = mesh.shape["gx"], mesh.shape["gy"]
    in_specs = (
        P("gx", "gy", None),
        P(("gx", "gy"), None),
        P(("gx", "gy")),
        P(("gx", "gy")),
        P(("gx", "gy"), None),
        P(),
        P(),
    )
    out_specs = (P(("gx", "gy")), P(), P("gx", "gy"))
    return jax.shard_map(
        functools.partial(local, n_gx, n_gy),
        mesh=mesh, in_specs=in_specs, out_specs=out_specs, check_vma=False,
    )
```

```python
import functools

import jax
import jax.numpy as jnp
from jax import lax
from jax.experimental import pallas as pl
from jax.experimental.pallas import tpu as pltpu
from jax.sharding import PartitionSpec as P

MESH = pl.DeviceIdType.MESH
F32 = jnp.float32
BF16 = jnp.bfloat16
NT = (((1,), (1,)), ((), ()))
LANES = 128
LAG = 3
STACK = 1
TAIL = 4
AHEAD = 5
FRONT = 0


def step_kernel(
    n_gx, n_gy, scale, tail,
    rows_hbm, probes_hbm, count_hbm, sensor_hbm, coef_hbm, owner_hbm, weights_hbm,
    owned_ref, new_ref, density_ref,
    count_ref, sensor_ref, rows_ref, coef_ref, owner_ref, weights_ref,
    small_sem,
    rows_sm, probes_ref, tile_ref, stage_ref, coef32_ref, send_ref, recv_ref, ids_send, ids_recv,
    mixer_ref, own_ref, part_out, part_in, part_x, acc_ref, planes_ref, h_send, h_recv,
    rows_sem, load_sem, send_sem, recv_sem, ids_send_sem, ids_recv_sem, part_send_sem,
    part_sem, part_x_sem, h_send_sem, h_recv_sem,
):
    n = n_gx * n_gy
    gx = lax.axis_index("gx")
    gy = lax.axis_index("gy")
    flat = gx * n_gy + gy
    groups, _, nblk, probe_n = send_ref.shape[1:]
    items, part_rows, width = part_in.shape[1:]
    tile_r, tile_c = probes_ref.shape[:2]
    split = probe_n // width
    stack = owner_ref.shape[1] // part_rows
    fine = split * stack
    depth_k = n_gx * nblk
    n_sens = owner_ref.shape[1]
    foot = coef_ref.shape[1]
    wide = ids_send.shape[1]
    share = wide // nblk
    first_tail = items - tail

    parts = load_sem.shape[0]
    span = tile_r // parts

    def load(q):
        at = pl.ds(q * span, span)
        return pltpu.make_async_copy(probes_hbm.at[at], probes_ref.at[at], load_sem.at[q])

    pairs = (
        (count_hbm, count_ref), (sensor_hbm, sensor_ref), (rows_hbm, rows_ref),
        (coef_hbm, coef_ref), (owner_hbm, owner_ref), (weights_hbm, weights_ref),
    )
    small = [
        pltpu.make_async_copy(src, dst, small_sem.at[i]) for i, (src, dst) in enumerate(pairs)
    ]
    for copy in small:
        copy.start()
    for q in range(parts):
        load(q).start()
    rows_copy = pltpu.make_async_copy(rows_hbm, rows_sm, rows_sem)
    rows_copy.start()

    def across(j):
        return (lax.rem(gx + j, n_gx), gy)

    barrier = pltpu.get_barrier_semaphore()

    def greet(j, carry):
        pl.semaphore_signal(barrier, inc=1, device_id=across(j), device_id_type=MESH)
        return carry

    lax.fori_loop(1, n_gx, greet, 0)

    @pl.when(gy > 0)
    def _():
        pl.semaphore_signal(barrier, inc=1, device_id=(gx, gy - 1), device_id_type=MESH)

    @pl.when(gy < n_gy - 1)
    def _():
        pl.semaphore_signal(barrier, inc=1, device_id=(gx, gy + 1), device_id_type=MESH)

    for q in range(parts):
        load(q).wait()

        def widen(i, carry):
            rows = probes_ref[i].astype(F32)
            for p in range(split):
                at = pl.ds(i * (tile_c * split) + p, tile_c, stride=split)
                tile_ref[at, :] = rows[:, p * width : (p + 1) * width]
            return carry

        lax.fori_loop(q * span, (q + 1) * span, widen, 0)
    for copy in small:
        copy.wait()
    coef32_ref[...] = coef_ref[...].astype(F32)
    slot = lax.broadcasted_iota(jnp.int32, (1, nblk), 1)
    ids_one = jnp.where(slot < count_ref[...], sensor_ref[...] + 1, 0).astype(F32)
    down = lax.broadcasted_iota(jnp.int32, (nblk, nblk), 0)
    ids_col = jnp.sum(
        jnp.where(down == lax.broadcasted_iota(jnp.int32, (nblk, nblk), 1), ids_one, 0.0),
        axis=1, keepdims=True,
    )
    offset = lax.rem(gx, share) * nblk
    ids_send[...] = jnp.sum(
        jnp.where(
            lax.broadcasted_iota(jnp.int32, (nblk, wide), 1)
            == lax.broadcasted_iota(jnp.int32, (nblk, wide), 0) + offset,
            ids_col, 0.0,
        ),
        axis=0, keepdims=True,
    )
    ids_recv[gx] = ids_send[...]

    def plane(j, carry):
        at = rows_ref[pl.ds(j, 1), :]
        c = coef32_ref[pl.ds(j, 1), :]
        square = c * c
        top = square.astype(BF16).astype(F32)
        high = at // tile_c
        low = at - high * tile_c
        here = high == lax.broadcasted_iota(jnp.int32, (tile_r, foot), 0)
        left = jnp.concatenate(
            [jnp.where(here, top, 0.0), jnp.where(here, square - top, 0.0)], axis=0
        ).astype(BF16)
        right = jnp.where(
            low == lax.broadcasted_iota(jnp.int32, (tile_c, foot), 0), 1.0, 0.0
        ).astype(BF16)
        both = lax.dot_general(left, right, NT, preferred_element_type=F32)
        planes_ref[j] = both[:tile_r] + both[tile_r:]
        return carry

    lax.fori_loop(0, FRONT, plane, 0)
    rows_copy.wait()

    def block_copy(q, g, j):
        return pltpu.make_async_remote_copy(
            src_ref=send_ref.at[q, g, across(j)[0]], dst_ref=recv_ref.at[q, g, gx],
            send_sem=send_sem, recv_sem=recv_sem.at[q, g],
            device_id=across(j), device_id_type=MESH,
        )

    def ids_copy(j):
        return pltpu.make_async_remote_copy(
            src_ref=ids_send, dst_ref=ids_recv.at[gx],
            send_sem=ids_send_sem, recv_sem=ids_recv_sem,
            device_id=across(j), device_id_type=MESH,
        )

    def part_copy(q, c, up):
        return pltpu.make_async_remote_copy(
            src_ref=part_out.at[q * items + c], dst_ref=part_in.at[q, c],
            send_sem=part_send_sem, recv_sem=part_sem.at[q, c],
            device_id=(gx, gy + up), device_id_type=MESH,
        )

    def part_x_copy(q, c, up):
        return pltpu.make_async_remote_copy(
            src_ref=part_out.at[q * items + c], dst_ref=part_x.at[q, c - first_tail],
            send_sem=part_send_sem, recv_sem=part_x_sem.at[q, c - first_tail],
            device_id=(gx, gy + up), device_id_type=MESH,
        )

    def h_peer(k):
        far = k // n_gx
        tz = jnp.where(gy < n_gy // 2, n_gy - 1 - far, far)
        tx = lax.rem(gx + lax.rem(k, n_gx), n_gx)
        return tx * n_gy + tz, (tx, tz)

    def h_copy(k):
        return pltpu.make_async_remote_copy(
            src_ref=h_send, dst_ref=h_recv.at[flat],
            send_sem=h_send_sem, recv_sem=h_recv_sem,
            device_id=h_peer(k)[1], device_id_type=MESH,
        )

    channel = lax.broadcasted_iota(jnp.int32, (nblk, foot), 1)
    batch = stage_ref.shape[0]

    def gather(q, g):
        def some(b, carry):
            for e in range(batch):
                d = b * batch + e
                r = (g * 2 + q) * n_gx + d
                column = jnp.sum(
                    jnp.where(channel == r, coef32_ref[...], 0.0), axis=1, keepdims=True
                )
                for j in range(nblk):
                    at = rows_sm[j, r] * split
                    stage_ref[e, pl.ds(j * split, split), :] = tile_ref[pl.ds(at, split), :]
                for p in range(split):
                    part = stage_ref[e, pl.ds(p, nblk, stride=split), :]
                    send_ref[q, g, d, :, p * width : (p + 1) * width] = (part * column).astype(BF16)
            return carry

        lax.fori_loop(0, n_gx // batch, some, 0)

    def launch(q, g):
        recv_ref[q, g, gx] = send_ref[q, g, gx]
        for j in range(1, n_gx):
            block_copy(q, g, j).start()

    pl.semaphore_wait(
        barrier,
        n_gx - 1 + jnp.where(gy > 0, 1, 0) + jnp.where(gy < n_gy - 1, 1, 0),
    )
    for j in range(1, n_gx):
        ids_copy(j).start()
    gather(0, 0)
    launch(0, 0)

    def gather_on(k, carry):
        gather(k % 2, k // 2)
        launch(k % 2, k // 2)
        return carry

    lax.fori_loop(1, AHEAD, gather_on, 0)

    rest = pl.ds(0, n_gx - 1)
    pltpu.make_async_copy(ids_recv.at[rest], ids_recv.at[rest], ids_recv_sem).wait()
    sensor_up = (lax.broadcasted_iota(jnp.int32, (n_sens, wide), 0) + 1).astype(F32)
    for piece in range(n_gx // share):
        row = ids_recv[piece * share]
        for extra in range(1, share):
            row = row + ids_recv[piece * share + extra]
        mixer_ref[:, piece * wide : (piece + 1) * wide] = jnp.where(
            row == sensor_up, 1.0, 0.0
        ).astype(BF16)
    acc_ref[...] = jnp.zeros_like(acc_ref)

    others = pl.ds(0, n_gx - 1)

    def mix(q, g):
        pltpu.make_async_copy(
            send_ref.at[q, g, others], recv_ref.at[q, g, others], recv_sem.at[q, g]
        ).wait()
        y = jnp.dot(
            mixer_ref[...], recv_ref[q, g].reshape(depth_k, probe_n), preferred_element_type=F32
        )
        for p in range(split):
            for v in range(stack):
                own_ref[q, (g * split + p) * stack + v] = y[
                    v * part_rows : (v + 1) * part_rows, p * width : (p + 1) * width
                ]

    def collect(q, c, f, crossing):
        below = (gy > 0) & (gy <= f)
        above = (gy < n_gy - 1) & (gy >= f)

        @pl.when(below if q == 0 else above)
        def _():
            pltpu.make_async_copy(part_out.at[0], part_in.at[q, c], part_sem.at[q, c]).wait()
            own_ref[q, c] += part_in[q, c].astype(F32)

        if crossing:
            @pl.when(above if q == 0 else below)
            def _():
                at = c - first_tail
                pltpu.make_async_copy(
                    part_out.at[0], part_x.at[q, at], part_x_sem.at[q, at]
                ).wait()
                own_ref[q, c] += part_x[q, at].astype(F32)

        @pl.when(gy == f)
        def _():
            v = lax.rem(c, stack)
            total = acc_ref[v]
            for at in range(0, width, LANES):
                y = own_ref[q, c, :, at : at + LANES]
                total = total + y * y
            acc_ref[v] = total

    def process(q, c, f, crossing, head):
        if not head:
            collect(q, c, f, crossing)

        @pl.when(gy < f)
        def _():
            part_out[q * items + c] = own_ref[q, c].astype(BF16)
            (part_copy if q == 0 else part_x_copy)(q, c, 1).start()

        @pl.when(gy > f)
        def _():
            part_out[q * items + c] = own_ref[q, c].astype(BF16)
            (part_copy if q == 1 else part_x_copy)(q, c, -1).start()

    def ends(q, crossing):
        if crossing:
            return n_gy // 2 - q
        return n_gy - 1 if q == 0 else 0

    def depth_of(f):
        low = jnp.where(gy <= f, gy, 0)
        high = jnp.where(gy >= f, n_gy - 1 - gy, 0)
        return jnp.maximum(low, high)

    late = fine // 2
    every, halves = max(1, fine // 2), max(1, 2 // fine)
    each = max(0, nblk - FRONT) // (2 * AHEAD)
    steps = items + late + LAG * (n_gy - 1)

    def turns(s, q, crossing):
        f = ends(q, crossing)
        lo, hi = (first_tail, items) if crossing else (0, first_tail)
        depth = depth_of(f)
        c = s - LAG * depth - (late if q else 0)
        return f, depth, c, (c >= lo) & (c < hi)

    kinds = (True, False) if tail else (False,)

    def chain(s):
        for crossing in reversed(kinds):
            for q in range(2):
                f, depth, c, turn = turns(s, q, crossing)

                @pl.when(turn & (depth > 0))
                def _():
                    process(q, c, f, crossing, False)

    def heads(s):
        for crossing in reversed(kinds):
            for q in range(2):
                f, depth, c, turn = turns(s, q, crossing)

                @pl.when(turn & (depth == 0) & ((gy == 0) if q == 0 else (gy > 0)))
                def _():
                    process(q, c, f, crossing, True)
        if tail:
            for q in range(2):
                f, depth, c, turn = turns(s - tail, q, True)

                @pl.when(turn & (depth == 0) & ((gy > 0) if q == 0 else (gy == 0)))
                def _():
                    process(q, c, f, True, True)

    def step(s, carry):
        chain(s)
        for e in range(halves):
            k = s // every * halves + e
            turn = lax.rem(s, every) == 0

            @pl.when(turn & (k + AHEAD < 2 * groups))
            def _():
                gather((k + AHEAD) % 2, (k + AHEAD) // 2)
                launch((k + AHEAD) % 2, (k + AHEAD) // 2)

            @pl.when(turn & (k + AHEAD >= 2 * groups) & (k < 2 * groups))
            def _():
                for b in range(each):
                    plane(FRONT + (k + AHEAD - 2 * groups) * each + b, 0)

            @pl.when(turn & (k < 2 * groups))
            def _():
                mix(k % 2, k // 2)

        heads(s)
        return carry

    lax.fori_loop(0, steps, step, 0)

    h_send[...] = lax.dot_general(
        jnp.ones((8, LANES), F32), acc_ref[...].reshape(n_sens, LANES), NT,
        precision=lax.Precision.HIGHEST, preferred_element_type=F32,
    )[0:1]
    h_recv[flat] = h_send[...]

    def h_launch(k, carry):
        @pl.when(h_peer(k)[0] != flat)
        def _():
            h_copy(k).start()
        return carry

    lax.fori_loop(0, n, h_launch, 0)
    lax.fori_loop(FRONT + AHEAD * each, nblk, plane, 0)

    spd = n_sens // n
    mine = jnp.where(owner_ref[...] == flat, 1.0, 0.0)
    before = jnp.where(
        lax.broadcasted_iota(jnp.int32, (n_sens, n_sens), 0)
        < lax.broadcasted_iota(jnp.int32, (n_sens, n_sens), 1),
        1.0, 0.0,
    ).astype(BF16)
    rank = jnp.dot(
        jnp.broadcast_to(mine, (spd, n_sens)).astype(BF16), before, preferred_element_type=F32
    )
    place = lax.broadcasted_iota(jnp.int32, (spd, n_sens), 0).astype(F32)
    select = jnp.where(rank == place, 1.0, 0.0) * mine

    def drain(count):
        sent = pl.ds(0, 2 * items - count)
        pltpu.make_async_copy(part_out.at[sent], part_out.at[sent], part_send_sem).wait()

    middle = (gy == n_gy // 2) | (gy == n_gy // 2 - 1)
    edge = (gy == 0) | (gy == n_gy - 1)
    pl.when(edge)(lambda: drain(first_tail))
    pl.when(middle & jnp.logical_not(edge))(lambda: drain(tail))
    pl.when(jnp.logical_not(middle | edge))(lambda: drain(0))
    whole = pl.ds(0, n_gx - 1)
    pltpu.make_async_copy(
        send_ref.at[:, :, whole], recv_ref.at[:, :, whole], send_sem
    ).wait()
    pltpu.make_async_copy(ids_recv.at[rest], ids_recv.at[rest], ids_send_sem).wait()

    peers = h_recv.at[pl.ds(0, n - 1)]
    pltpu.make_async_copy(peers, peers, h_send_sem).wait()
    pltpu.make_async_copy(peers, peers, h_recv_sem).wait()
    h = jnp.sum(h_recv[...], axis=0) * scale
    gain = weights_ref[...] * jnp.sqrt(1.0 + h)
    new = n_sens * gain / jnp.sum(gain, axis=1, keepdims=True)
    new_ref[...] = new
    owned = jnp.sum(select * h, axis=1, keepdims=True)
    small = lax.broadcasted_iota(jnp.int32, (spd, spd), 0) == lax.broadcasted_iota(
        jnp.int32, (spd, spd), 1
    )
    owned_ref[...] = jnp.sum(jnp.where(small, owned, 0.0), axis=0, keepdims=True)
    lookup = ids_col == (lax.broadcasted_iota(jnp.int32, (nblk, n_sens), 1) + 1).astype(F32)
    factor = jnp.sum(jnp.where(lookup, new, 0.0), axis=1, keepdims=True)
    total = factor[0:1] * planes_ref[0]
    for j in range(1, nblk):
        total = total + factor[j : j + 1] * planes_ref[j]
    density_ref[...] = total


def write_kernel(owned_in, new_in, density_in, owned_ref, new_ref, density_ref):
    owned_ref[...] = owned_in[...]
    new_ref[...] = new_in[...]
    density_ref[...] = density_in[...]


def local(n_gx, n_gy, probes, blk_rows, blk_sensor, blk_count, coef, owner, weights):
    tile_r, tile_c, probe_n = probes.shape
    nblk, foot = blk_rows.shape
    n_sens = owner.shape[0]
    n = n_gx * n_gy
    width = LANES
    groups, split = foot // n_gx // 2, probe_n // width
    stack = STACK
    part_rows = n_sens // stack
    items = groups * split * stack
    tail = TAIL * items // 32 if n_gy > 3 else 0
    wide = max(LANES, nblk)
    batch = min(n_gx, max(1, 256 // nblk))

    vmem = pl.BlockSpec(memory_space=pltpu.VMEM)
    hbm = pl.BlockSpec(memory_space=pltpu.HBM)
    dma = pltpu.SemaphoreType.DMA
    outs = (
        jax.ShapeDtypeStruct((1, n_sens // n), F32),
        jax.ShapeDtypeStruct((1, n_sens), F32),
        jax.ShapeDtypeStruct((tile_r, tile_c), F32),
    )
    results = pl.pallas_call(
        functools.partial(step_kernel, n_gx, n_gy, 1.0 / (foot * probe_n), tail),
        out_shape=tuple(pltpu.VMEM(out.shape, out.dtype) for out in outs),
        in_specs=[hbm] * 7,
        out_specs=(vmem,) * 3,
        scratch_shapes=[
            pltpu.VMEM((1, 1), jnp.int32),
            pltpu.VMEM((1, nblk), jnp.int32),
            pltpu.VMEM((nblk, foot), jnp.int32),
            pltpu.VMEM((nblk, foot), BF16),
            pltpu.VMEM((1, n_sens), jnp.int32),
            pltpu.VMEM((1, n_sens), F32),
            dma((6,)),
            pltpu.SMEM((nblk, foot), jnp.int32),
            pltpu.VMEM((tile_r, tile_c, probe_n), BF16),
            pltpu.VMEM((tile_r * tile_c * split, width), F32),
            pltpu.VMEM((batch, nblk * split, width), F32),
            pltpu.VMEM((nblk, foot), F32),
            pltpu.VMEM((2, groups, n_gx, nblk, probe_n), BF16),
            pltpu.VMEM((2, groups, n_gx, nblk, probe_n), BF16),
            pltpu.VMEM((1, wide), F32),
            pltpu.VMEM((n_gx, 1, wide), F32),
            pltpu.VMEM((n_sens, n_gx * nblk), BF16),
            pltpu.VMEM((2, items, part_rows, width), F32),
            pltpu.VMEM((2 * items, part_rows, width), BF16),
            pltpu.VMEM((2, items, part_rows, width), BF16),
            pltpu.VMEM((2, max(1, tail), part_rows, width), BF16),
            pltpu.VMEM((stack, part_rows, LANES), F32),
            pltpu.VMEM((nblk, tile_r, tile_c), F32),
            pltpu.VMEM((1, n_sens), F32),
            pltpu.VMEM((n, 1, n_sens), F32),
            dma, dma((4,)), dma, dma((2, groups)), dma, dma, dma,
            dma((2, items)), dma((2, max(1, tail))), dma, dma,
        ],
        compiler_params=pltpu.CompilerParams(
            collective_id=0, has_side_effects=True, vmem_limit_bytes=60 * 2**20
        ),
        name="reweight_step",
    )(
        blk_rows, probes, blk_count.reshape(1, 1), blk_sensor.reshape(1, nblk), coef,
        owner.reshape(1, n_sens), weights.reshape(1, n_sens),
    )
    owned, new, density = pl.pallas_call(
        write_kernel,
        out_shape=outs,
        in_specs=[vmem] * 3,
        out_specs=(vmem,) * 3,
        name="write_results",
    )(*[pltpu.with_memory_space_constraint(r, pltpu.VMEM) for r in results])
    return owned.reshape(-1), new.reshape(-1), density


def solution(mesh):
    n_gx, n_gy = mesh.shape["gx"], mesh.shape["gy"]
    in_specs = (
        P("gx", "gy", None),
        P(("gx", "gy"), None),
        P(("gx", "gy")),
        P(("gx", "gy")),
        P(("gx", "gy"), None),
        P(),
        P(),
    )
    out_specs = (P(("gx", "gy")), P(), P("gx", "gy"))
    return jax.shard_map(
        functools.partial(local, n_gx, n_gy),
        mesh=mesh, in_specs=in_specs, out_specs=out_specs, check_vma=False,
    )
```
